32 devices in a mesh: pa: 8 (over z, x), sa: 4 (over y, core).
Axes of the slice: x: 2, y: 2, z: 4, core: 2. Of those that a mesh axis runs over, the one named last changes fastest.
Arguments:
- factors: bfloat16 [64, 16, 1024], P(None, None, 'pa'), may hold values from -6 to 6
- trade_weights: bfloat16 [64, 8192], P(None, 'pa'), may hold values from -0.75 to 0.75
- payoff_terms: bfloat16 [2, 8192], P(None, 'pa'), may hold values from -6 to 6
- set_blocks: int32 [32], replicated, may hold values from 1 to 4, 64 in all
- shock_pick: int32 [8], P('sa'), may hold values from 0 to 31
- shock_scale: float32 [32, 64], replicated, may hold values from 0.25 to 1.75
- shock_shift: float32 [32, 64], replicated, may hold values from -3 to 3
- discount: bfloat16 [16, 1024], P(None, 'pa'), may hold values from 0.5 to 1
- set_pd: float32 [32, 16], P('pa'), may hold values from 0.02 to 0.2
- own_pd: float32 [16], replicated, may hold values from 0.02 to 0.2
Outputs:
- exposure_profile: float32 [2, 32, 16, 8], P(None, 'pa', None, 'sa')
- set_xva: float32 [32, 8], P('pa', 'sa')
- total_xva: float32 [8], P('sa')
The draws below stay inside these ranges and needn't reach their ends.
Inputs may be any that keep to these rules, and one draw needn't show every extreme that they name: `set_blocks`: each of the 32 netting sets holds whole consecutive blocks of 128 trades; the counts sum to 64.
All inputs are finite; a program needn't handle non-finite values.
Results may differ from the reference program's by a relative error of at most 0.00046.
Values may be sent and summed in bfloat16 or wider, within the bound.
A program may use at most 64 MiB of HBM per device.

```python
import math
import jax
import jax.numpy as jnp
import numpy as np
from jax import lax

K = 64
TRADES = 8192
TBLOCKS = 64
NSETS = 32
LIB = 32
DATES = 16
SHOCKS = 8
PATHS = 1024


def with_ends(values, key, smallest, top_value):
    dims = values.shape
    place = [jax.random.randint(jax.random.fold_in(key, axis), (), 0, dims[axis]) for axis in range(len(dims))]
    values = values.at[tuple(place)].set(smallest)
    longest = dims.index(max(dims))
    place[longest] = (place[longest] + 1) % dims[longest]
    return values.at[tuple(place)].set(top_value)


def shard_levels(stream_key, extent, pieces, low, high):
    loudness = 1.0
    for axis_at, shards_of in pieces:
        steps = jax.random.uniform(jax.random.fold_in(jax.random.fold_in(stream_key, 6), axis_at), (shards_of,), jnp.float32, low / len(pieces), high / len(pieces))
        loudness = loudness * jnp.repeat(jnp.exp(steps), extent[axis_at] // shards_of).reshape((-1,) + (1,) * (len(extent) - 1 - axis_at))
    return loudness


def split_up(number_of, total, most, skew):
    weights = [(1 << 20) // math.isqrt(rank ** skew) + 1 for rank in range(2, number_of + 1)]
    spare, holding = total - most - (number_of - 1), [1] * (number_of - 1)
    while spare > 0:
        candidates = [i for i in range(number_of - 1) if holding[i] < most]
        whole, left = sum([weights[i] for i in candidates]), spare
        for i in candidates:
            more = min(most - holding[i], max(1, left * weights[i] // whole), spare)
            holding[i] = holding[i] + more
            spare = spare - more
    return np.array([most] + holding)


def ragged(own_key, amount, total, reach, lean):
    if amount == 2:
        one = jax.random.randint(own_key, (), max(1, total - reach), min(reach, total - 1) + 1)
        return jnp.stack([one, total - one])
    lengths = jnp.asarray(split_up(amount, total, reach, lean), jnp.int32)
    pairs = (amount - 1) // 2
    donor, receiver = lengths[1:1 + 2 * pairs:2], lengths[2:2 + 2 * pairs:2]
    slack = jnp.minimum(donor - 1, reach - receiver)
    shifted = jax.random.randint(jax.random.fold_in(own_key, 1), (pairs,), 0, 1 << 20) % (slack + 1)
    lengths = lengths.at[1:1 + 2 * pairs:2].set(donor - shifted).at[2:2 + 2 * pairs:2].set(receiver + shifted)
    return lengths[jax.random.permutation(jax.random.fold_in(own_key, 2), amount)]


def gaussian(own_key, dims, scale, bound, pieces=(), kind=jnp.bfloat16):
    values = scale * jax.random.normal(own_key, dims, jnp.float32)
    if pieces:
        values = values * shard_levels(own_key, dims, pieces, -0.22, 0.18)
    return jnp.clip(values, -bound, bound).astype(kind)


def setup_inputs(seed: int = 0) -> dict:
    key_of = jax.random.split(jax.random.key(seed), 11)
    factors = gaussian(key_of[0], (K, DATES, PATHS), 1.0, 6.0, ((2, 8),))
    trade_weights = gaussian(key_of[1], (K, TRADES), K ** -0.5, 0.75, ((1, 8),))
    payoff_terms = gaussian(key_of[2], (2, TRADES), 1.0, 6.0, ((1, 8),))
    set_blocks = ragged(key_of[3], NSETS, TBLOCKS, 4, 2).astype(jnp.int32)
    shock_pick = with_ends(jax.random.randint(key_of[4], (SHOCKS,), 0, LIB), jax.random.fold_in(key_of[4], 1), 0, LIB - 1).astype(jnp.int32)
    shock_scale = jnp.clip(1.0 + 0.15 * jax.random.normal(key_of[5], (LIB, K), jnp.float32), 0.25, 1.75)
    shock_shift = gaussian(key_of[6], (LIB, K), 0.5, 3.0, (), jnp.float32)
    discount = jnp.clip(jnp.exp(math.log(1.0) - 0.6931472 * jax.random.uniform(key_of[7], (DATES, PATHS), jnp.float32) ** shard_levels(key_of[7], (DATES, PATHS), ((1, 8),), -0.2, 0.2)), 0.5, 1.0).astype(jnp.bfloat16)
    set_pd = jnp.clip(jnp.exp(math.log(0.2) - 2.3025851 * jax.random.uniform(key_of[8], (NSETS, DATES), jnp.float32) ** shard_levels(key_of[8], (NSETS, DATES), ((0, 8),), -0.2, 0.2)), 0.02, 0.2)
    own_pd = jnp.clip(jnp.exp(jax.random.uniform(key_of[9], (DATES,), jnp.float32, math.log(0.02), math.log(0.2))), 0.02, 0.2)
    return dict(factors=factors, trade_weights=trade_weights, payoff_terms=payoff_terms, set_blocks=set_blocks, shock_pick=shock_pick, shock_scale=shock_scale, shock_shift=shock_shift, discount=discount, set_pd=set_pd, own_pd=own_pd)


UNIT_SCALE = 0.0625


def trade_members(set_blocks):
    set_ends = jnp.cumsum(set_blocks).astype(jnp.int32)
    block_ids = jnp.arange(TBLOCKS, dtype=jnp.int32)
    owners = jnp.sum((set_ends[None, :] <= block_ids[:, None]).astype(jnp.int32), axis=1).astype(jnp.int32)
    trade_owner = jnp.repeat(owners, 128)
    set_ids = jnp.arange(NSETS, dtype=jnp.int32)
    return (trade_owner[None, :] == set_ids[:, None]).astype(jnp.bfloat16)


def reference(factors, trade_weights, payoff_terms, set_blocks, shock_pick, shock_scale, shock_shift, discount, set_pd, own_pd):
    members = trade_members(set_blocks)
    library = jnp.arange(LIB, dtype=jnp.int32)
    pick_rows = (shock_pick[:, None] == library[None, :]).astype(jnp.float32)
    scale_rows = jnp.dot(pick_rows, shock_scale, precision=lax.Precision.HIGHEST)
    shift_rows = jnp.dot(pick_rows, shock_shift, precision=lax.Precision.HIGHEST)
    notional = payoff_terms[0].astype(jnp.float32)[:, None]
    strike = payoff_terms[1].astype(jnp.float32)[:, None]

    def one_pair(position):
        date_index = position // SHOCKS
        shock_index = position % SHOCKS
        date_factors = lax.dynamic_index_in_dim(factors, date_index, 1, False).astype(jnp.float32)
        scale_one = lax.dynamic_index_in_dim(scale_rows, shock_index, 0, False)
        shift_one = lax.dynamic_index_in_dim(shift_rows, shock_index, 0, False)
        shocked = (scale_one[:, None] * date_factors + shift_one[:, None]).astype(jnp.bfloat16)
        levels = lax.dot_general(trade_weights, shocked, (((0,), (0,)), ((), ())), preferred_element_type=jnp.float32)
        values = (notional * jax.nn.softplus(levels + strike)).astype(jnp.bfloat16)
        netted = UNIT_SCALE * jnp.dot(members, values, preferred_element_type=jnp.float32)
        date_discount = lax.dynamic_index_in_dim(discount, date_index, 0, False).astype(jnp.float32)
        exposure = netted * date_discount[None, :]
        positive = jnp.sum(jnp.maximum(exposure, 0.0), axis=1) / PATHS
        negative = jnp.sum(jnp.minimum(exposure, 0.0), axis=1) / PATHS
        return jnp.stack([positive, negative])

    results = lax.map(one_pair, jnp.arange(DATES * SHOCKS, dtype=jnp.int32))
    profile = results.reshape(DATES, SHOCKS, 2, NSETS).transpose(2, 3, 0, 1)
    adjustment = jnp.sum(set_pd[:, :, None] * profile[0], axis=1) + jnp.sum(own_pd[None, :, None] * profile[1], axis=1)
    set_xva = adjustment - jnp.sum(adjustment, axis=1, keepdims=True) / SHOCKS
    total_xva = jnp.sum(adjustment, axis=0)
    return profile, set_xva, total_xva
```

```python
import functools
import math

import jax
import jax.numpy as jnp
from jax import lax
from jax.experimental import pallas as pl
from jax.experimental.pallas import tpu as pltpu
from jax.sharding import PartitionSpec as P

UNIT_SCALE = 0.0625
LOG2E = 1.0 / math.log(2.0)
BLOCK = 128
BF = jnp.bfloat16
F32 = jnp.float32
CEIL = 100.0
KDIM = 128
SUB = 128


def pick_column(library_ref, row):
    count, width = library_ref.shape
    rows = lax.broadcasted_iota(jnp.int32, (count, width), 0)
    line = jnp.sum(jnp.where(rows == row, library_ref[...], 0.0), axis=0, keepdims=True)
    square = jnp.broadcast_to(line, (width, width))
    eye = lax.broadcasted_iota(jnp.int32, (width, width), 0) == lax.broadcasted_iota(
        jnp.int32, (width, width), 1
    )
    return jnp.sum(jnp.where(eye, square, 0.0), axis=1, keepdims=True)


def shock_rows(factor_ref, pick_ref, scale_ref, shift_ref, wide_ref, shocked_ref):
    factors, dates, paths = factor_ref.shape
    shocks = pick_ref.shape[0]
    for k in range(factors):
        wide_ref[k * dates : (k + 1) * dates, :] = factor_ref[k].astype(F32)
    rest = shocked_ref.shape[0] - factors
    ones = lax.broadcasted_iota(jnp.int32, (rest, shocked_ref.shape[1]), 0) < 2
    shocked_ref[factors:, :] = jnp.where(ones, 1.0, 0.0).astype(BF)
    for s in range(shocks):
        scale = pick_column(scale_ref, pick_ref[s]) * LOG2E
        shift = pick_column(shift_ref, pick_ref[s]) * LOG2E
        scale = jnp.broadcast_to(scale, (factors, paths))
        shift = jnp.broadcast_to(shift, (factors, paths))
        for d in range(dates):
            line = wide_ref[pl.ds(d, factors, stride=dates), :]
            at = (d * shocks + s) * paths
            shocked_ref[:factors, at : at + paths] = (scale * line + shift).astype(BF)


def load_trades(weights, terms, factors):
    strike = terms[1:2].astype(F32) * LOG2E
    high = strike.astype(BF).astype(F32)
    low = strike - high
    width = weights.shape[1]
    rest = jnp.zeros((KDIM - factors - 8, width), F32)
    row = lax.broadcasted_iota(jnp.int32, (8, width), 0)
    tail = jnp.where(row == 0, high, jnp.where(row == 1, low, 0.0))
    stack = jnp.concatenate([weights.astype(F32), tail, rest], axis=0)
    return stack.T.astype(BF)


def send(source, target, send_sem, recv_sem, place):
    return pltpu.make_async_remote_copy(
        src_ref=source,
        dst_ref=target,
        send_sem=send_sem,
        recv_sem=recv_sem,
        device_id=place,
        device_id_type=pl.DeviceIdType.MESH,
    )


def kernel(
    groups,
    lanes_across,
    pick_ref,
    factor_ref,
    weight_ref,
    term_ref,
    block_ref,
    scale_ref,
    shift_ref,
    discount_ref,
    pd_ref,
    own_ref,
    out_ref,
    wide_ref,
    shocked_ref,
    loading_ref,
    member_ref,
    net_ref,
    weight_all,
    term_all,
    pd_all,
    message_ref,
    inbox_ref,
    send_sem,
    recv_sem,
    post_sem,
    inbox_sem,
):
    factors, dates, paths = factor_ref.shape
    shocks = pick_ref.shape[0]
    local = weight_ref.shape[1]
    sets = block_ref.shape[1]
    owned = pd_ref.shape[0]
    across = lanes_across
    devices = groups * across
    me_p = lax.axis_index("pa")
    me_s = lax.axis_index("sa")
    me = me_p * across + me_s
    parts = ((weight_ref, weight_all), (term_ref, term_all), (pd_ref, pd_all))

    barrier = pltpu.get_barrier_semaphore()

    def greet(step, _):
        other = lax.rem(me + step, devices)
        pl.semaphore_signal(
            barrier,
            inc=1,
            device_id=(other // across, lax.rem(other, across)),
            device_id_type=pl.DeviceIdType.MESH,
        )
        return 0

    lax.fori_loop(1, devices, greet, 0)
    for n, (source, target) in enumerate(parts):
        pltpu.make_async_copy(source, target.at[me_p], recv_sem.at[n, me_p]).start()
    shock_rows(factor_ref, pick_ref, scale_ref, shift_ref, wide_ref, shocked_ref)
    pl.semaphore_wait(barrier, devices - 1)

    def gather(step):
        other = lax.rem(me_p - step + groups, groups)
        return [
            send(source, target.at[me_p], send_sem.at[n, step], recv_sem.at[n, me_p], (other, me_s))
            for n, (source, target) in enumerate(parts)
        ]

    for step in range(1, groups):
        for copy in gather(step):
            copy.start()

    m = lax.broadcasted_iota(jnp.int32, (sets, sets), 0)
    j = lax.broadcasted_iota(jnp.int32, (sets, sets), 1)
    counts = jnp.broadcast_to(block_ref[...].astype(F32), (sets, sets))
    ends = jnp.sum(jnp.where(j <= m, counts, 0.0), axis=1, keepdims=True) * BLOCK
    begins = jnp.sum(jnp.where(j < m, counts, 0.0), axis=1, keepdims=True) * BLOCK
    net_ref[...] = jnp.zeros_like(net_ref)
    wide = shocks * paths
    unroll = 8 if dates % 8 == 0 else 1
    sub = min(SUB, local)

    def one_slot(step, _):
        slot = lax.rem(me_p + step, groups)
        for n, (source, target) in enumerate(parts):
            pltpu.make_async_copy(source, target.at[slot], recv_sem.at[n, slot]).wait()
        terms = term_all[slot]
        loading_ref[...] = load_trades(weight_all[slot], terms, factors)
        ids = lax.broadcasted_iota(jnp.int32, (sets, local), 1) + slot * local
        ids = ids.astype(F32)
        notional = jnp.broadcast_to(terms[0:1].astype(F32), (sets, local))
        inside = jnp.logical_and(ids >= begins, ids < ends)
        member_ref[...] = jnp.where(inside, notional, 0.0).astype(BF)

        def some_dates(turn, _):
            for d in range(unroll):
                at = pl.multiple_of((turn * unroll + d) * wide, wide)
                columns = shocked_ref[:, pl.ds(at, wide)]
                values = []
                for r in range(0, local, sub):
                    part = loading_ref[r : r + sub, :]
                    u = jnp.dot(part, columns, preferred_element_type=F32)
                    grown = jnp.exp2(jnp.minimum(u, CEIL))
                    values.append(jnp.maximum(jnp.log2(grown + 1.0), u).astype(BF))
                whole = jnp.concatenate(values, axis=0)
                net_ref[:, pl.ds(at, wide)] += jnp.dot(
                    member_ref[...], whole, preferred_element_type=F32
                )
            return 0

        lax.fori_loop(0, dates // unroll, some_dates, 0)
        return 0

    lax.fori_loop(0, groups, one_slot, 0)

    count = dates * shocks
    lane = lax.broadcasted_iota(jnp.int32, (sets, 128), 1)
    sums = jnp.zeros((sets, 128), F32)
    total_paths = paths * groups
    for d in range(dates):
        cheap = discount_ref[d : d + 1, :].astype(F32) * (UNIT_SCALE * math.log(2.0))
        for s in range(shocks):
            at = d * wide + s * paths
            exposure = net_ref[:, at : at + paths] * cheap
            up = jnp.sum(jnp.maximum(exposure, 0.0), axis=1, keepdims=True)
            down = jnp.sum(jnp.minimum(exposure, 0.0), axis=1, keepdims=True)
            sums = jnp.where(lane == s * dates + d, up, sums)
            sums = jnp.where(lane == count + s * dates + d, down, sums)
    sums = sums / total_paths

    rest = jnp.zeros((owned, 128 - 2 * count), F32)
    own = [jnp.broadcast_to(own_ref[...], (owned, dates))] * shocks
    small = lax.broadcasted_iota(jnp.int32, (owned, 128), 1)

    def of_shock(s):
        up = jnp.logical_and(small >= s * dates, small < (s + 1) * dates)
        down = jnp.logical_and(small >= count + s * dates, small < count + (s + 1) * dates)
        return jnp.logical_or(up, down)

    totals = [jnp.zeros((1, 1), F32)] * shocks
    blocks = []
    for q in range(groups):
        rows = sums[q * owned : (q + 1) * owned, :]
        prices = jnp.concatenate([pd_all[q]] * shocks + own + [rest], axis=1)
        part = prices * rows
        both = jnp.sum(part, axis=1, keepdims=True)
        blocks.append(jnp.where(small == 2 * count, both, rows))
        for s in range(shocks):
            picked = jnp.sum(jnp.where(of_shock(s), part, 0.0), axis=1, keepdims=True)
            totals[s] = totals[s] + jnp.sum(picked, axis=0, keepdims=True)
    for q in range(groups):
        block = blocks[q]
        for s in range(shocks):
            block = jnp.where(small == 2 * count + 1 + s, totals[s], block)
        message_ref[q] = block
    inbox_ref[me_p, me_s] = message_ref[me_p]

    def post(step):
        other = lax.rem(me + step, devices)
        other_p = other // across
        return send(
            message_ref.at[other_p],
            inbox_ref.at[me_p, me_s],
            post_sem.at[step],
            inbox_sem.at[me],
            (other_p, lax.rem(other, across)),
        )

    def post_one(step, _):
        post(step).start()
        return 0

    def take_one(step, _):
        source = lax.rem(me + step, devices)
        pltpu.make_async_copy(
            message_ref.at[0],
            inbox_ref.at[source // across, lax.rem(source, across)],
            inbox_sem.at[source],
        ).wait()
        return 0

    def done_one(step, _):
        post(step).wait_send()
        return 0

    lax.fori_loop(1, devices, post_one, 0)
    for step in range(1, groups):
        for copy in gather(step):
            copy.wait_send()
    lax.fori_loop(1, devices, take_one, 0)

    mine = jnp.zeros((owned, 128), F32)
    every = jnp.zeros((owned, 128), F32)
    for q in range(groups):
        mine = mine + inbox_ref[q, me_s]
        for s in range(across):
            every = every + inbox_ref[q, s]
    mean = jnp.sum(jnp.where(small == 2 * count, every, 0.0), axis=1, keepdims=True)
    mean = mean / (shocks * across)
    part = jnp.concatenate([pd_ref[...]] * shocks + own + [rest], axis=1) * mine
    for s in range(shocks):
        adjustment = jnp.sum(jnp.where(of_shock(s), part, 0.0), axis=1, keepdims=True)
        mine = jnp.where(small == 2 * count + 1 + shocks + s, adjustment - mean, mine)
    out_ref[...] = mine
    lax.fori_loop(1, devices, done_one, 0)


def on_device(
    factors,
    trade_weights,
    payoff_terms,
    set_blocks,
    shock_pick,
    shock_scale,
    shock_shift,
    discount,
    set_pd,
    own_pd,
):
    sets = set_blocks.shape[0]
    owned = set_pd.shape[0]
    count, dates, paths = factors.shape
    shocks = shock_pick.shape[0]
    groups = lax.axis_size("pa")
    across = lax.axis_size("sa")
    local = trade_weights.shape[1]
    vmem = pl.BlockSpec(memory_space=pltpu.VMEM)
    smem = pl.BlockSpec(memory_space=pltpu.SMEM)
    result = pl.pallas_call(
        functools.partial(kernel, groups, across),
        out_shape=jax.ShapeDtypeStruct((owned, 128), F32),
        in_specs=[smem] + [vmem] * 9,
        out_specs=vmem,
        scratch_shapes=[
            pltpu.VMEM((count * dates, paths), F32),
            pltpu.VMEM((KDIM, dates * shocks * paths), BF),
            pltpu.VMEM((local, KDIM), BF),
            pltpu.VMEM((sets, local), BF),
            pltpu.VMEM((sets, dates * shocks * paths), F32),
            pltpu.VMEM((groups,) + trade_weights.shape, BF),
            pltpu.VMEM((groups,) + payoff_terms.shape, BF),
            pltpu.VMEM((groups,) + set_pd.shape, F32),
            pltpu.VMEM((groups, owned, 128), F32),
            pltpu.VMEM((groups, across, owned, 128), F32),
            pltpu.SemaphoreType.DMA((3, groups)),
            pltpu.SemaphoreType.DMA((3, groups)),
            pltpu.SemaphoreType.DMA((groups * across,)),
            pltpu.SemaphoreType.DMA((groups * across,)),
        ],
        compiler_params=pltpu.CompilerParams(
            vmem_limit_bytes=48 * 1024 * 1024, collective_id=0, has_side_effects=True
        ),
    )(
        shock_pick,
        factors,
        trade_weights,
        payoff_terms,
        set_blocks[None, :],
        shock_scale,
        shock_shift,
        discount,
        set_pd,
        own_pd[None, :],
    )
    lanes = dates * shocks
    profile = result[:, : 2 * lanes].reshape(owned, 2, shocks, dates)
    profile = profile.transpose(1, 0, 3, 2)
    total_xva = result[0, 2 * lanes + 1 : 2 * lanes + 1 + shocks]
    set_xva = result[:, 2 * lanes + 1 + shocks : 2 * lanes + 1 + 2 * shocks]
    return (profile, set_xva, total_xva)


def solution(mesh):
    return jax.shard_map(
        on_device,
        mesh=mesh,
        in_specs=(
            P(None, None, "pa"),
            P(None, "pa"),
            P(None, "pa"),
            P(),
            P("sa"),
            P(),
            P(),
            P(None, "pa"),
            P("pa", None),
            P(),
        ),
        out_specs=(P(None, "pa", None, "sa"), P("pa", "sa"), P("sa")),
        check_vma=False,
    )
```

```python
import functools
import math

import jax
import jax.numpy as jnp
from jax import lax
from jax.experimental import pallas as pl
from jax.experimental.pallas import tpu as pltpu
from jax.sharding import PartitionSpec as P

UNIT_SCALE = 0.0625
LOG2E = 1.0 / math.log(2.0)
BLOCK = 128
BF = jnp.bfloat16
F32 = jnp.float32
CEIL = 100.0
KDIM = 128
SUB = 128


def pick_column(library_ref, row):
    count, width = library_ref.shape
    rows = lax.broadcasted_iota(jnp.int32, (count, width), 0)
    line = jnp.sum(jnp.where(rows == row, library_ref[...], 0.0), axis=0, keepdims=True)
    square = jnp.broadcast_to(line, (width, width))
    eye = lax.broadcasted_iota(jnp.int32, (width, width), 0) == lax.broadcasted_iota(
        jnp.int32, (width, width), 1
    )
    return jnp.sum(jnp.where(eye, square, 0.0), axis=1, keepdims=True)


def shock_rows(factor_ref, pick_ref, scale_ref, shift_ref, wide_ref, shocked_ref):
    factors, dates, paths = factor_ref.shape
    shocks = pick_ref.shape[0]
    for k in range(factors):
        wide_ref[k * dates : (k + 1) * dates, :] = factor_ref[k].astype(F32)
    rest = shocked_ref.shape[0] - factors
    ones = lax.broadcasted_iota(jnp.int32, (rest, shocked_ref.shape[1]), 0) < 2
    shocked_ref[factors:, :] = jnp.where(ones, 1.0, 0.0).astype(BF)
    for s in range(shocks):
        scale = pick_column(scale_ref, pick_ref[s]) * LOG2E
        shift = pick_column(shift_ref, pick_ref[s]) * LOG2E
        scale = jnp.broadcast_to(scale, (factors, paths))
        shift = jnp.broadcast_to(shift, (factors, paths))
        for d in range(dates):
            line = wide_ref[pl.ds(d, factors, stride=dates), :]
            at = (d * shocks + s) * paths
            shocked_ref[:factors, at : at + paths] = (scale * line + shift).astype(BF)


def load_trades(weights, terms, factors):
    strike = terms[1:2].astype(F32) * LOG2E
    high = strike.astype(BF).astype(F32)
    low = strike - high
    width = weights.shape[1]
    rest = jnp.zeros((KDIM - factors - 8, width), F32)
    row = lax.broadcasted_iota(jnp.int32, (8, width), 0)
    tail = jnp.where(row == 0, high, jnp.where(row == 1, low, 0.0))
    stack = jnp.concatenate([weights.astype(F32), tail, rest], axis=0)
    return stack.T.astype(BF)


def partner(me, step, groups):
    if groups & (groups - 1):
        return lax.rem(me + step, groups)
    other, bit = 0, 1
    while bit < groups:
        other = other + lax.rem(me // bit + step // bit, 2) * bit
        bit = bit * 2
    return other


def send(source, target, send_sem, recv_sem, place):
    return pltpu.make_async_remote_copy(
        src_ref=source,
        dst_ref=target,
        send_sem=send_sem,
        recv_sem=recv_sem,
        device_id=place,
        device_id_type=pl.DeviceIdType.MESH,
    )


def kernel(
    groups,
    lanes_across,
    pick_hbm,
    factor_hbm,
    weight_hbm,
    term_hbm,
    block_hbm,
    scale_hbm,
    shift_hbm,
    discount_hbm,
    pd_hbm,
    own_hbm,
    out_ref,
    pick_ref,
    factor_ref,
    block_ref,
    scale_ref,
    shift_ref,
    discount_ref,
    own_ref,
    wide_ref,
    shocked_ref,
    loading_ref,
    member_ref,
    net_ref,
    weight_all,
    term_all,
    pd_all,
    message_ref,
    inbox_ref,
    send_sem,
    recv_sem,
    post_sem,
    inbox_sem,
    load_sem,
):
    factors, dates, paths = factor_ref.shape
    shocks = pick_ref.shape[0]
    local = weight_hbm.shape[1]
    sets = block_ref.shape[1]
    owned = pd_hbm.shape[0]
    across = lanes_across
    devices = groups * across
    me_p = lax.axis_index("pa")
    me_s = lax.axis_index("sa")
    me = me_p * across + me_s
    parts = ((weight_hbm, weight_all), (term_hbm, term_all), (pd_hbm, pd_all))
    early = [
        pltpu.make_async_copy(source, target, load_sem.at[n])
        for n, (source, target) in enumerate(
            (
                (pick_hbm, pick_ref),
                (scale_hbm, scale_ref),
                (shift_hbm, shift_ref),
                (factor_hbm, factor_ref),
                (block_hbm, block_ref),
                (discount_hbm, discount_ref),
                (own_hbm, own_ref),
            )
        )
    ]
    for copy in early:
        copy.start()
    for n, (source, target) in enumerate(parts):
        pltpu.make_async_copy(source, target.at[me_p], recv_sem.at[n, me_p]).start()

    barrier = pltpu.get_barrier_semaphore()

    def greet(step, _):
        other = lax.rem(me + step, devices)
        pl.semaphore_signal(
            barrier,
            inc=1,
            device_id=(other // across, lax.rem(other, across)),
            device_id_type=pl.DeviceIdType.MESH,
        )
        return 0

    lax.fori_loop(1, devices, greet, 0)
    for copy in early:
        copy.wait()
    shock_rows(factor_ref, pick_ref, scale_ref, shift_ref, wide_ref, shocked_ref)

    def gather(step):
        other = partner(me_p, step if not groups & (groups - 1) else groups - step, groups)
        return [
            send(
                target.at[me_p],
                target.at[me_p],
                send_sem.at[n, step],
                recv_sem.at[n, me_p],
                (other, me_s),
            )
            for n, (source, target) in enumerate(parts)
        ]

    m = lax.broadcasted_iota(jnp.int32, (sets, sets), 0)
    j = lax.broadcasted_iota(jnp.int32, (sets, sets), 1)
    counts = jnp.broadcast_to(block_ref[...].astype(F32), (sets, sets))
    ends = jnp.sum(jnp.where(j <= m, counts, 0.0), axis=1, keepdims=True) * BLOCK
    begins = jnp.sum(jnp.where(j < m, counts, 0.0), axis=1, keepdims=True) * BLOCK
    net_ref[...] = jnp.zeros_like(net_ref)
    wide = shocks * paths
    unroll = 8 if dates % 8 == 0 else 1
    sub = min(SUB, local)

    def one_slot(step, _):
        slot = partner(me_p, step, groups)
        for n, (source, target) in enumerate(parts):
            pltpu.make_async_copy(source, target.at[slot], recv_sem.at[n, slot]).wait()
        terms = term_all[slot]
        loading_ref[...] = load_trades(weight_all[slot], terms, factors)
        ids = lax.broadcasted_iota(jnp.int32, (sets, local), 1) + slot * local
        ids = ids.astype(F32)
        notional = jnp.broadcast_to(terms[0:1].astype(F32), (sets, local))
        inside = jnp.logical_and(ids >= begins, ids < ends)
        member_ref[...] = jnp.where(inside, notional, 0.0).astype(BF)

        def some_dates(turn, _):
            for d in range(unroll):
                at = pl.multiple_of((turn * unroll + d) * wide, wide)
                columns = shocked_ref[:, pl.ds(at, wide)]
                values = []
                for r in range(0, local, sub):
                    part = loading_ref[r : r + sub, :]
                    u = jnp.dot(part, columns, preferred_element_type=F32)
                    grown = jnp.exp2(jnp.minimum(u, CEIL))
                    values.append(jnp.maximum(jnp.log2(grown + 1.0), u).astype(BF))
                whole = jnp.concatenate(values, axis=0)
                net_ref[:, pl.ds(at, wide)] += jnp.dot(
                    member_ref[...], whole, preferred_element_type=F32
                )

            @pl.when(jnp.logical_and(step == 0, turn == 0))
            def _():
                pl.semaphore_wait(barrier, devices - 1)
                for ahead in range(1, groups):
                    for copy in gather(ahead):
                        copy.start()

            return 0

        lax.fori_loop(0, dates // unroll, some_dates, 0)
        return 0

    lax.fori_loop(0, groups, one_slot, 0)

    count = dates * shocks
    lane = lax.broadcasted_iota(jnp.int32, (sets, 128), 1)
    sums = jnp.zeros((sets, 128), F32)
    total_paths = paths * groups
    for d in range(dates):
        cheap = discount_ref[d : d + 1, :].astype(F32) * (UNIT_SCALE * math.log(2.0))
        for s in range(shocks):
            at = d * wide + s * paths
            exposure = net_ref[:, at : at + paths] * cheap
            up = jnp.sum(jnp.maximum(exposure, 0.0), axis=1, keepdims=True)
            down = jnp.sum(jnp.minimum(exposure, 0.0), axis=1, keepdims=True)
            sums = jnp.where(lane == s * dates + d, up, sums)
            sums = jnp.where(lane == count + s * dates + d, down, sums)
    sums = sums / total_paths

    rest = jnp.zeros((owned, 128 - 2 * count), F32)
    own = [jnp.broadcast_to(own_ref[...], (owned, dates))] * shocks
    small = lax.broadcasted_iota(jnp.int32, (owned, 128), 1)

    def of_shock(s):
        up = jnp.logical_and(small >= s * dates, small < (s + 1) * dates)
        down = jnp.logical_and(small >= count + s * dates, small < count + (s + 1) * dates)
        return jnp.logical_or(up, down)

    totals = [jnp.zeros((1, 1), F32)] * shocks
    blocks = []
    for q in range(groups):
        rows = sums[q * owned : (q + 1) * owned, :]
        prices = jnp.concatenate([pd_all[q]] * shocks + own + [rest], axis=1)
        part = prices * rows
        both = jnp.sum(part, axis=1, keepdims=True)
        blocks.append(jnp.where(small == 2 * count, both, rows))
        for s in range(shocks):
            picked = jnp.sum(jnp.where(of_shock(s), part, 0.0), axis=1, keepdims=True)
            totals[s] = totals[s] + jnp.sum(picked, axis=0, keepdims=True)
    for q in range(groups):
        block = blocks[q]
        for s in range(shocks):
            block = jnp.where(small == 2 * count + 1 + s, totals[s], block)
        message_ref[q] = block
    inbox_ref[me_p, me_s] = message_ref[me_p]

    def post(step):
        other = lax.rem(me + step, devices)
        other_p = other // across
        return send(
            message_ref.at[other_p],
            inbox_ref.at[me_p, me_s],
            post_sem.at[step],
            inbox_sem.at[me],
            (other_p, lax.rem(other, across)),
        )

    def post_one(step, _):
        post(step).start()
        return 0

    def take_one(step, _):
        source = lax.rem(me + step, devices)
        pltpu.make_async_copy(
            message_ref.at[0],
            inbox_ref.at[source // across, lax.rem(source, across)],
            inbox_sem.at[source],
        ).wait()
        return 0

    def done_one(step, _):
        post(step).wait_send()
        return 0

    lax.fori_loop(1, devices, post_one, 0)
    for step in range(1, groups):
        for copy in gather(step):
            copy.wait_send()
    lax.fori_loop(1, devices, take_one, 0)

    mine = jnp.zeros((owned, 128), F32)
    every = jnp.zeros((owned, 128), F32)
    for q in range(groups):
        mine = mine + inbox_ref[q, me_s]
        for s in range(across):
            every = every + inbox_ref[q, s]
    mean = jnp.sum(jnp.where(small == 2 * count, every, 0.0), axis=1, keepdims=True)
    mean = mean / (shocks * across)
    part = jnp.concatenate([pd_all[me_p]] * shocks + own + [rest], axis=1) * mine
    for s in range(shocks):
        adjustment = jnp.sum(jnp.where(of_shock(s), part, 0.0), axis=1, keepdims=True)
        mine = jnp.where(small == 2 * count + 1 + shocks + s, adjustment - mean, mine)
    out_ref[...] = mine
    lax.fori_loop(1, devices, done_one, 0)


def on_device(
    factors,
    trade_weights,
    payoff_terms,
    set_blocks,
    shock_pick,
    shock_scale,
    shock_shift,
    discount,
    set_pd,
    own_pd,
):
    sets = set_blocks.shape[0]
    owned = set_pd.shape[0]
    count, dates, paths = factors.shape
    shocks = shock_pick.shape[0]
    groups = lax.axis_size("pa")
    across = lax.axis_size("sa")
    local = trade_weights.shape[1]
    vmem = pl.BlockSpec(memory_space=pltpu.VMEM)
    hbm = pl.BlockSpec(memory_space=pltpu.HBM)
    result = pl.pallas_call(
        functools.partial(kernel, groups, across),
        out_shape=jax.ShapeDtypeStruct((owned, 128), F32),
        in_specs=[hbm] * 10,
        out_specs=vmem,
        scratch_shapes=[
            pltpu.SMEM(shock_pick.shape, jnp.int32),
            pltpu.VMEM(factors.shape, BF),
            pltpu.VMEM((1, sets), jnp.int32),
            pltpu.VMEM(shock_scale.shape, F32),
            pltpu.VMEM(shock_shift.shape, F32),
            pltpu.VMEM(discount.shape, BF),
            pltpu.VMEM((1, dates), F32),
            pltpu.VMEM((count * dates, paths), F32),
            pltpu.VMEM((KDIM, dates * shocks * paths), BF),
            pltpu.VMEM((local, KDIM), BF),
            pltpu.VMEM((sets, local), BF),
            pltpu.VMEM((sets, dates * shocks * paths), F32),
            pltpu.VMEM((groups,) + trade_weights.shape, BF),
            pltpu.VMEM((groups,) + payoff_terms.shape, BF),
            pltpu.VMEM((groups,) + set_pd.shape, F32),
            pltpu.VMEM((groups, owned, 128), F32),
            pltpu.VMEM((groups, across, owned, 128), F32),
            pltpu.SemaphoreType.DMA((3, groups)),
            pltpu.SemaphoreType.DMA((3, groups)),
            pltpu.SemaphoreType.DMA((groups * across,)),
            pltpu.SemaphoreType.DMA((groups * across,)),
            pltpu.SemaphoreType.DMA((7,)),
        ],
        compiler_params=pltpu.CompilerParams(
            collective_id=0, has_side_effects=True
        ),
    )(
        shock_pick,
        factors,
        trade_weights,
        payoff_terms,
        set_blocks[None, :],
        shock_scale,
        shock_shift,
        discount,
        set_pd,
        own_pd[None, :],
    )
    lanes = dates * shocks
    profile = result[:, : 2 * lanes].reshape(owned, 2, shocks, dates)
    profile = profile.transpose(1, 0, 3, 2)
    total_xva = result[0, 2 * lanes + 1 : 2 * lanes + 1 + shocks]
    set_xva = result[:, 2 * lanes + 1 + shocks : 2 * lanes + 1 + 2 * shocks]
    return (profile, set_xva, total_xva)


def solution(mesh):
    return jax.shard_map(
        on_device,
        mesh=mesh,
        in_specs=(
            P(None, None, "pa"),
            P(None, "pa"),
            P(None, "pa"),
            P(),
            P("sa"),
            P(),
            P(),
            P(None, "pa"),
            P("pa", None),
            P(),
        ),
        out_specs=(P(None, "pa", None, "sa"), P("pa", "sa"), P("sa")),
        check_vma=False,
    )
```

```python
import functools
import math

import jax
import jax.numpy as jnp
from jax import lax
from jax.experimental import pallas as pl
from jax.experimental.pallas import tpu as pltpu
from jax.sharding import PartitionSpec as P

UNIT_SCALE = 0.0625
LOG2E = 1.0 / math.log(2.0)
BLOCK = 128
BF = jnp.bfloat16
F32 = jnp.float32
CEIL = 100.0
KDIM = 128
SUB = 128


def pick_column(library_ref, row):
    count, width = library_ref.shape
    rows = lax.broadcasted_iota(jnp.int32, (count, width), 0)
    line = jnp.sum(jnp.where(rows == row, library_ref[...], 0.0), axis=0, keepdims=True)
    square = jnp.broadcast_to(line, (width, width))
    eye = lax.broadcasted_iota(jnp.int32, (width, width), 0) == lax.broadcasted_iota(
        jnp.int32, (width, width), 1
    )
    return jnp.sum(jnp.where(eye, square, 0.0), axis=1, keepdims=True)


def shock_rows(factor_ref, pick_ref, scale_ref, shift_ref, wide_ref, shocked_ref):
    factors, dates, paths = factor_ref.shape
    shocks = pick_ref.shape[0]
    for k in range(factors):
        wide_ref[k * dates : (k + 1) * dates, :] = factor_ref[k].astype(F32)
    rest = shocked_ref.shape[0] - factors
    ones = lax.broadcasted_iota(jnp.int32, (rest, shocked_ref.shape[1]), 0) < 2
    shocked_ref[factors:, :] = jnp.where(ones, 1.0, 0.0).astype(BF)
    for s in range(shocks):
        scale = pick_column(scale_ref, pick_ref[s]) * LOG2E
        shift = pick_column(shift_ref, pick_ref[s]) * LOG2E
        scale = jnp.broadcast_to(scale, (factors, paths))
        shift = jnp.broadcast_to(shift, (factors, paths))
        for d in range(dates):
            line = wide_ref[pl.ds(d, factors, stride=dates), :]
            at = (d * shocks + s) * paths
            shocked_ref[:factors, at : at + paths] = (scale * line + shift).astype(BF)


def load_trades(weights, terms, factors):
    strike = terms[1:2].astype(F32) * LOG2E
    high = strike.astype(BF).astype(F32)
    low = strike - high
    width = weights.shape[1]
    row = lax.broadcasted_iota(jnp.int32, (KDIM - factors, width), 0)
    tail = jnp.where(row == 0, high, jnp.where(row == 1, low, 0.0)).astype(BF)
    return jnp.concatenate([weights, tail], axis=0).T


def partner(me, step, groups):
    if groups & (groups - 1):
        return lax.rem(me + step, groups)
    other, bit = 0, 1
    while bit < groups:
        other = other + lax.rem(me // bit + step // bit, 2) * bit
        bit = bit * 2
    return other


def send(source, target, send_sem, recv_sem, place):
    return pltpu.make_async_remote_copy(
        src_ref=source,
        dst_ref=target,
        send_sem=send_sem,
        recv_sem=recv_sem,
        device_id=place,
        device_id_type=pl.DeviceIdType.MESH,
    )


def kernel(
    groups,
    lanes_across,
    pick_hbm,
    factor_hbm,
    weight_hbm,
    term_hbm,
    block_hbm,
    scale_hbm,
    shift_hbm,
    discount_hbm,
    pd_hbm,
    own_hbm,
    profile_ref,
    xva_ref,
    total_ref,
    pick_ref,
    factor_ref,
    block_ref,
    scale_ref,
    shift_ref,
    discount_ref,
    own_ref,
    wide_ref,
    shocked_ref,
    loading_ref,
    member_ref,
    net_ref,
    weight_all,
    term_all,
    pd_all,
    message_ref,
    inbox_ref,
    send_sem,
    recv_sem,
    post_sem,
    inbox_sem,
    load_sem,
):
    factors, dates, paths = factor_ref.shape
    shocks = pick_ref.shape[0]
    local = weight_hbm.shape[1]
    sets = block_ref.shape[1]
    owned = pd_hbm.shape[0]
    across = lanes_across
    devices = groups * across
    me_p = lax.axis_index("pa")
    me_s = lax.axis_index("sa")
    me = me_p * across + me_s
    parts = ((weight_hbm, weight_all), (term_hbm, term_all), (pd_hbm, pd_all))
    early = [
        pltpu.make_async_copy(source, target, load_sem.at[n])
        for n, (source, target) in enumerate(
            (
                (pick_hbm, pick_ref),
                (scale_hbm, scale_ref),
                (shift_hbm, shift_ref),
                (factor_hbm, factor_ref),
                (block_hbm, block_ref),
                (discount_hbm, discount_ref),
                (own_hbm, own_ref),
            )
        )
    ]
    for copy in early:
        copy.start()
    for n, (source, target) in enumerate(parts):
        pltpu.make_async_copy(source, target.at[me_p], recv_sem.at[n, me_p]).start()

    barrier = pltpu.get_barrier_semaphore()

    def greet(place):
        pl.semaphore_signal(
            barrier, inc=1, device_id=place, device_id_type=pl.DeviceIdType.MESH
        )

    for step in range(1, groups):
        greet((lax.rem(me_p + step, groups), me_s))
    for step in range(1, across):
        greet((me_p, lax.rem(me_s + step, across)))
    for copy in early:
        copy.wait()
    shock_rows(factor_ref, pick_ref, scale_ref, shift_ref, wide_ref, shocked_ref)

    def gather(step):
        other = partner(me_p, step if not groups & (groups - 1) else groups - step, groups)
        return [
            send(
                target.at[me_p],
                target.at[me_p],
                send_sem.at[n, step],
                recv_sem.at[n, me_p],
                (other, me_s),
            )
            for n, (source, target) in enumerate(parts)
        ]

    for n, (source, target) in enumerate(parts):
        pltpu.make_async_copy(source, target.at[me_p], recv_sem.at[n, me_p]).wait()
    pl.semaphore_wait(barrier, groups + across - 2)
    for step in range(1, groups):
        for copy in gather(step):
            copy.start()

    m = lax.broadcasted_iota(jnp.int32, (sets, sets), 0)
    j = lax.broadcasted_iota(jnp.int32, (sets, sets), 1)
    counts = jnp.broadcast_to(block_ref[...].astype(F32), (sets, sets))
    ends = jnp.sum(jnp.where(j <= m, counts, 0.0), axis=1, keepdims=True) * BLOCK
    begins = jnp.sum(jnp.where(j < m, counts, 0.0), axis=1, keepdims=True) * BLOCK
    net_ref[...] = jnp.zeros_like(net_ref)
    wide = shocks * paths
    unroll = next(n for n in (16, 8, 4, 2, 1) if dates % n == 0)
    sub = min(SUB, local)

    def one_slot(step, _):
        slot = partner(me_p, step, groups)

        @pl.when(step > 0)
        def _():
            for n, (source, target) in enumerate(parts):
                pltpu.make_async_copy(source, target.at[slot], recv_sem.at[n, slot]).wait()

        terms = term_all[slot]
        loading_ref[...] = load_trades(weight_all[slot], terms, factors)
        ids = lax.broadcasted_iota(jnp.int32, (sets, local), 1) + slot * local
        ids = ids.astype(F32)
        notional = jnp.broadcast_to(terms[0:1].astype(F32), (sets, local))
        inside = jnp.logical_and(ids >= begins, ids < ends)
        member_ref[...] = jnp.where(inside, notional, 0.0).astype(BF)

        def some_dates(turn, _):
            for d in range(unroll):
                at = pl.multiple_of((turn * unroll + d) * wide, wide)
                columns = shocked_ref[:, pl.ds(at, wide)]
                values = []
                for r in range(0, local, sub):
                    part = loading_ref[r : r + sub, :]
                    u = jnp.dot(part, columns, preferred_element_type=F32)
                    grown = jnp.exp2(jnp.minimum(u, CEIL))
                    values.append(jnp.maximum(jnp.log2(grown + 1.0), u).astype(BF))
                whole = jnp.concatenate(values, axis=0)
                net_ref[:, pl.ds(at, wide)] += jnp.dot(
                    member_ref[...], whole, preferred_element_type=F32
                )
            return 0

        lax.fori_loop(0, dates // unroll, some_dates, 0)
        return 0

    lax.fori_loop(0, groups, one_slot, 0)

    count = dates * shocks
    lane = lax.broadcasted_iota(jnp.int32, (sets, 128), 1)
    sums = jnp.zeros((sets, 128), F32)
    total_paths = paths * groups
    for d in range(dates):
        cheap = discount_ref[d : d + 1, :].astype(F32) * (UNIT_SCALE * math.log(2.0))
        for s in range(shocks):
            at = d * wide + s * paths
            exposure = net_ref[:, at : at + paths] * cheap
            up = jnp.sum(jnp.maximum(exposure, 0.0), axis=1, keepdims=True)
            down = jnp.sum(jnp.minimum(exposure, 0.0), axis=1, keepdims=True)
            sums = jnp.where(lane == s * dates + d, up, sums)
            sums = jnp.where(lane == count + s * dates + d, down, sums)
    sums = sums / total_paths

    rest = jnp.zeros((owned, 128 - 2 * count), F32)
    own = [jnp.broadcast_to(own_ref[...], (owned, dates))] * shocks
    small = lax.broadcasted_iota(jnp.int32, (owned, 128), 1)

    def of_shock(s):
        up = jnp.logical_and(small >= s * dates, small < (s + 1) * dates)
        down = jnp.logical_and(small >= count + s * dates, small < count + (s + 1) * dates)
        return jnp.logical_or(up, down)

    totals = [jnp.zeros((1, 1), F32)] * shocks
    blocks = []
    for q in range(groups):
        rows = sums[q * owned : (q + 1) * owned, :]
        prices = jnp.concatenate([pd_all[q]] * shocks + own + [rest], axis=1)
        part = prices * rows
        both = jnp.sum(part, axis=1, keepdims=True)
        blocks.append(jnp.where(small == 2 * count, both, rows))
        for s in range(shocks):
            picked = jnp.sum(jnp.where(of_shock(s), part, 0.0), axis=1, keepdims=True)
            totals[s] = totals[s] + jnp.sum(picked, axis=0, keepdims=True)
    for q in range(groups):
        block = blocks[q]
        for s in range(shocks):
            block = jnp.where(small == 2 * count + 1 + s, totals[s], block)
        message_ref[q] = block
    inbox_ref[me_p, me_s] = message_ref[me_p]

    def post(step):
        other = lax.rem(me + step, devices)
        other_p = other // across
        return send(
            message_ref.at[other_p],
            inbox_ref.at[me_p, me_s],
            post_sem.at[step],
            inbox_sem.at[me],
            (other_p, lax.rem(other, across)),
        )

    def post_one(step, _):
        post(step).start()
        return 0

    def take_one(step, _):
        source = lax.rem(me + step, devices)
        pltpu.make_async_copy(
            message_ref.at[0],
            inbox_ref.at[source // across, lax.rem(source, across)],
            inbox_sem.at[source],
        ).wait()
        return 0

    def done_one(step, _):
        post(step).wait_send()
        return 0

    lax.fori_loop(1, devices, post_one, 0)
    for step in range(1, groups):
        for copy in gather(step):
            copy.wait_send()
    lax.fori_loop(1, devices, take_one, 0)

    mine = jnp.zeros((owned, 128), F32)
    every = jnp.zeros((owned, 128), F32)
    for q in range(groups):
        mine = mine + inbox_ref[q, me_s]
        for s in range(across):
            every = every + inbox_ref[q, s]
    mean = jnp.sum(jnp.where(small == 2 * count, every, 0.0), axis=1, keepdims=True)
    mean = mean / (shocks * across)
    part = jnp.concatenate([pd_all[me_p]] * shocks + own + [rest], axis=1) * mine
    for half in range(2):
        for s in range(shocks):
            at = half * count + s * dates
            profile_ref[half, :, s, :] = mine[:, at : at + dates]
    diagonal = small == lax.broadcasted_iota(jnp.int32, (owned, 128), 0)
    for s in range(shocks):
        adjustment = jnp.sum(jnp.where(of_shock(s), part, 0.0), axis=1, keepdims=True)
        line = jnp.sum(jnp.where(diagonal, adjustment - mean, 0.0), axis=0, keepdims=True)
        xva_ref[s : s + 1, :] = line[:, :owned]
    at = 2 * count + 1
    total_ref[...] = mine[0:1, at : at + shocks]
    lax.fori_loop(1, devices, done_one, 0)


def on_device(
    factors,
    trade_weights,
    payoff_terms,
    set_blocks,
    shock_pick,
    shock_scale,
    shock_shift,
    discount,
    set_pd,
    own_pd,
):
    sets = set_blocks.shape[0]
    owned = set_pd.shape[0]
    count, dates, paths = factors.shape
    shocks = shock_pick.shape[0]
    groups = lax.axis_size("pa")
    across = lax.axis_size("sa")
    local = trade_weights.shape[1]
    vmem = pl.BlockSpec(memory_space=pltpu.VMEM)
    hbm = pl.BlockSpec(memory_space=pltpu.HBM)
    profile, set_xva, total_xva = pl.pallas_call(
        functools.partial(kernel, groups, across),
        out_shape=(
            jax.ShapeDtypeStruct((2, owned, shocks, dates), F32),
            jax.ShapeDtypeStruct((shocks, owned), F32),
            jax.ShapeDtypeStruct((1, shocks), F32),
        ),
        in_specs=[hbm] * 10,
        out_specs=(vmem, vmem, vmem),
        scratch_shapes=[
            pltpu.SMEM(shock_pick.shape, jnp.int32),
            pltpu.VMEM(factors.shape, BF),
            pltpu.VMEM((1, sets), jnp.int32),
            pltpu.VMEM(shock_scale.shape, F32),
            pltpu.VMEM(shock_shift.shape, F32),
            pltpu.VMEM(discount.shape, BF),
            pltpu.VMEM((1, dates), F32),
            pltpu.VMEM((count * dates, paths), F32),
            pltpu.VMEM((KDIM, dates * shocks * paths), BF),
            pltpu.VMEM((local, KDIM), BF),
            pltpu.VMEM((sets, local), BF),
            pltpu.VMEM((sets, dates * shocks * paths), F32),
            pltpu.VMEM((groups,) + trade_weights.shape, BF),
            pltpu.VMEM((groups,) + payoff_terms.shape, BF),
            pltpu.VMEM((groups,) + set_pd.shape, F32),
            pltpu.VMEM((groups, owned, 128), F32),
            pltpu.VMEM((groups, across, owned, 128), F32),
            pltpu.SemaphoreType.DMA((3, groups)),
            pltpu.SemaphoreType.DMA((3, groups)),
            pltpu.SemaphoreType.DMA((groups * across,)),
            pltpu.SemaphoreType.DMA((groups * across,)),
            pltpu.SemaphoreType.DMA((7,)),
        ],
        compiler_params=pltpu.CompilerParams(
            collective_id=0, has_side_effects=True
        ),
    )(
        shock_pick,
        factors,
        trade_weights,
        payoff_terms,
        set_blocks[None, :],
        shock_scale,
        shock_shift,
        discount,
        set_pd,
        own_pd[None, :],
    )
    return (profile.transpose(0, 1, 3, 2), set_xva.T, total_xva[0])


def solution(mesh):
    return jax.shard_map(
        on_device,
        mesh=mesh,
        in_specs=(
            P(None, None, "pa"),
            P(None, "pa"),
            P(None, "pa"),
            P(),
            P("sa"),
            P(),
            P(),
            P(None, "pa"),
            P("pa", None),
            P(),
        ),
        out_specs=(P(None, "pa", None, "sa"), P("pa", "sa"), P("sa")),
        check_vma=False,
    )
```

```python
import functools
import math

import jax
import jax.numpy as jnp
from jax import lax
from jax.experimental import pallas as pl
from jax.experimental.pallas import tpu as pltpu
from jax.sharding import PartitionSpec as P

UNIT_SCALE = 0.0625
LOG2E = 1.0 / math.log(2.0)
BLOCK = 128
BF = jnp.bfloat16
F32 = jnp.float32
CEIL = 100.0
KDIM = 128
SUB = 128


def pick_column(library_ref, row):
    count, width = library_ref.shape
    rows = lax.broadcasted_iota(jnp.int32, (count, width), 0)
    line = jnp.sum(jnp.where(rows == row, library_ref[...], 0.0), axis=0, keepdims=True)
    square = jnp.broadcast_to(line, (width, width))
    eye = lax.broadcasted_iota(jnp.int32, (width, width), 0) == lax.broadcasted_iota(
        jnp.int32, (width, width), 1
    )
    return jnp.sum(jnp.where(eye, square, 0.0), axis=1, keepdims=True)


def shock_rows(factor_ref, pick_ref, scale_ref, shift_ref, wide_ref, shocked_ref):
    factors, dates, paths = factor_ref.shape
    shocks = pick_ref.shape[0]
    for k in range(factors):
        wide_ref[k * dates : (k + 1) * dates, :] = factor_ref[k].astype(F32)
    rest = shocked_ref.shape[0] - factors
    ones = lax.broadcasted_iota(jnp.int32, (rest, shocked_ref.shape[1]), 0) < 2
    shocked_ref[factors:, :] = jnp.where(ones, 1.0, 0.0).astype(BF)
    for s in range(shocks):
        scale = pick_column(scale_ref, pick_ref[s]) * LOG2E
        shift = pick_column(shift_ref, pick_ref[s]) * LOG2E
        scale = jnp.broadcast_to(scale, (factors, paths))
        shift = jnp.broadcast_to(shift, (factors, paths))
        for d in range(dates):
            line = wide_ref[pl.ds(d, factors, stride=dates), :]
            at = (d * shocks + s) * paths
            shocked_ref[:factors, at : at + paths] = (scale * line + shift).astype(BF)


def load_trades(weights, terms, factors):
    strike = terms[1:2].astype(F32) * LOG2E
    high = strike.astype(BF).astype(F32)
    low = strike - high
    width = weights.shape[1]
    row = lax.broadcasted_iota(jnp.int32, (KDIM - factors, width), 0)
    tail = jnp.where(row == 0, high, jnp.where(row == 1, low, 0.0)).astype(BF)
    return jnp.concatenate([weights, tail], axis=0).T


def partner(me, step, groups):
    if groups & (groups - 1):
        return lax.rem(me + step, groups)
    other, bit = 0, 1
    while bit < groups:
        other = other + lax.rem(me // bit + step // bit, 2) * bit
        bit = bit * 2
    return other


def send(source, target, send_sem, recv_sem, place):
    return pltpu.make_async_remote_copy(
        src_ref=source,
        dst_ref=target,
        send_sem=send_sem,
        recv_sem=recv_sem,
        device_id=place,
        device_id_type=pl.DeviceIdType.MESH,
    )


def kernel(
    groups,
    lanes_across,
    pick_hbm,
    factor_hbm,
    weight_hbm,
    term_hbm,
    block_hbm,
    scale_hbm,
    shift_hbm,
    discount_hbm,
    pd_hbm,
    own_hbm,
    out_ref,
    pick_ref,
    factor_ref,
    block_ref,
    scale_ref,
    shift_ref,
    discount_ref,
    own_ref,
    wide_ref,
    shocked_ref,
    loading_ref,
    member_ref,
    net_ref,
    weight_all,
    term_all,
    pd_all,
    message_ref,
    inbox_ref,
    send_sem,
    recv_sem,
    post_sem,
    inbox_sem,
    load_sem,
):
    factors, dates, paths = factor_ref.shape
    shocks = pick_ref.shape[0]
    local = weight_hbm.shape[1]
    sets = block_ref.shape[1]
    owned = pd_hbm.shape[0]
    across = lanes_across
    devices = groups * across
    me_p = lax.axis_index("pa")
    me_s = lax.axis_index("sa")
    me = me_p * across + me_s
    parts = ((weight_hbm, weight_all), (term_hbm, term_all), (pd_hbm, pd_all))
    early = [
        pltpu.make_async_copy(source, target, load_sem.at[n])
        for n, (source, target) in enumerate(
            (
                (pick_hbm, pick_ref),
                (scale_hbm, scale_ref),
                (shift_hbm, shift_ref),
                (factor_hbm, factor_ref),
                (block_hbm, block_ref),
                (discount_hbm, discount_ref),
                (own_hbm, own_ref),
            )
        )
    ]
    for copy in early:
        copy.start()
    for n, (source, target) in enumerate(parts):
        pltpu.make_async_copy(source, target.at[me_p], recv_sem.at[n, me_p]).start()

    barrier = pltpu.get_barrier_semaphore()

    def greet(place):
        pl.semaphore_signal(
            barrier, inc=1, device_id=place, device_id_type=pl.DeviceIdType.MESH
        )

    for step in range(1, groups):
        greet((lax.rem(me_p + step, groups), me_s))
    for step in range(1, across):
        greet((me_p, lax.rem(me_s + step, across)))
    def gather(step):
        other = partner(me_p, step if not groups & (groups - 1) else groups - step, groups)
        return [
            send(
                target.at[me_p],
                target.at[me_p],
                send_sem.at[n, step],
                recv_sem.at[n, me_p],
                (other, me_s),
            )
            for n, (source, target) in enumerate(parts)
        ]

    for n, (source, target) in enumerate(parts):
        pltpu.make_async_copy(source, target.at[me_p], recv_sem.at[n, me_p]).wait()
    pl.semaphore_wait(barrier, groups + across - 2)
    for step in range(1, groups):
        for copy in gather(step):
            copy.start()
    for copy in early:
        copy.wait()
    shock_rows(factor_ref, pick_ref, scale_ref, shift_ref, wide_ref, shocked_ref)

    m = lax.broadcasted_iota(jnp.int32, (sets, sets), 0)
    j = lax.broadcasted_iota(jnp.int32, (sets, sets), 1)
    counts = jnp.broadcast_to(block_ref[...].astype(F32), (sets, sets))
    ends = jnp.sum(jnp.where(j <= m, counts, 0.0), axis=1, keepdims=True) * BLOCK
    begins = jnp.sum(jnp.where(j < m, counts, 0.0), axis=1, keepdims=True) * BLOCK
    net_ref[...] = jnp.zeros_like(net_ref)
    wide = shocks * paths
    unroll = next(n for n in (16, 8, 4, 2, 1) if dates % n == 0)
    sub = min(SUB, local)

    def one_slot(step, _):
        slot = partner(me_p, step, groups)

        @pl.when(step > 0)
        def _():
            for n, (source, target) in enumerate(parts):
                pltpu.make_async_copy(source, target.at[slot], recv_sem.at[n, slot]).wait()

        terms = term_all[slot]
        loading_ref[...] = load_trades(weight_all[slot], terms, factors)
        ids = lax.broadcasted_iota(jnp.int32, (sets, local), 1) + slot * local
        ids = ids.astype(F32)
        notional = jnp.broadcast_to(terms[0:1].astype(F32), (sets, local))
        inside = jnp.logical_and(ids >= begins, ids < ends)
        member_ref[...] = jnp.where(inside, notional, 0.0).astype(BF)

        def some_dates(turn, _):
            for d in range(unroll):
                at = pl.multiple_of((turn * unroll + d) * wide, wide)
                columns = shocked_ref[:, pl.ds(at, wide)]
                values = []
                for r in range(0, local, sub):
                    part = loading_ref[r : r + sub, :]
                    u = jnp.dot(part, columns, preferred_element_type=F32)
                    grown = jnp.exp2(jnp.minimum(u, CEIL))
                    values.append(jnp.maximum(jnp.log2(grown + 1.0), u).astype(BF))
                whole = jnp.concatenate(values, axis=0)
                net_ref[:, pl.ds(at, wide)] += jnp.dot(
                    member_ref[...], whole, preferred_element_type=F32
                )
            return 0

        lax.fori_loop(0, dates // unroll, some_dates, 0)
        return 0

    lax.fori_loop(0, groups, one_slot, 0)

    count = dates * shocks
    lane = lax.broadcasted_iota(jnp.int32, (sets, 128), 1)
    sums = jnp.zeros((sets, 128), F32)
    total_paths = paths * groups
    for d in range(dates):
        cheap = discount_ref[d : d + 1, :].astype(F32) * (UNIT_SCALE * math.log(2.0))
        for s in range(shocks):
            at = d * wide + s * paths
            exposure = net_ref[:, at : at + paths] * cheap
            up = jnp.sum(jnp.maximum(exposure, 0.0), axis=1, keepdims=True)
            down = jnp.sum(jnp.minimum(exposure, 0.0), axis=1, keepdims=True)
            sums = jnp.where(lane == s * dates + d, up, sums)
            sums = jnp.where(lane == count + s * dates + d, down, sums)
    sums = sums / total_paths

    rest = jnp.zeros((owned, 128 - 2 * count), F32)
    own = [jnp.broadcast_to(own_ref[...], (owned, dates))] * shocks
    small = lax.broadcasted_iota(jnp.int32, (owned, 128), 1)

    def of_shock(s):
        up = jnp.logical_and(small >= s * dates, small < (s + 1) * dates)
        down = jnp.logical_and(small >= count + s * dates, small < count + (s + 1) * dates)
        return jnp.logical_or(up, down)

    totals = [jnp.zeros((1, 1), F32)] * shocks
    blocks = []
    for q in range(groups):
        rows = sums[q * owned : (q + 1) * owned, :]
        prices = jnp.concatenate([pd_all[q]] * shocks + own + [rest], axis=1)
        part = prices * rows
        both = jnp.sum(part, axis=1, keepdims=True)
        blocks.append(jnp.where(small == 2 * count, both, rows))
        for s in range(shocks):
            picked = jnp.sum(jnp.where(of_shock(s), part, 0.0), axis=1, keepdims=True)
            totals[s] = totals[s] + jnp.sum(picked, axis=0, keepdims=True)
    for q in range(groups):
        block = blocks[q]
        for s in range(shocks):
            block = jnp.where(small == 2 * count + 1 + s, totals[s], block)
        message_ref[q] = block
    inbox_ref[me] = message_ref[me_p]

    for far_p in reversed(range(groups)):
        for far_s in reversed(range(across)):
            if far_p + far_s:
                other_p = partner(me_p, far_p, groups)
                send(
                    message_ref.at[other_p],
                    inbox_ref.at[me],
                    post_sem,
                    inbox_sem,
                    (other_p, partner(me_s, far_s, across)),
                ).start()
    for step in range(1, groups):
        for copy in gather(step):
            copy.wait_send()
    others = inbox_ref.at[pl.ds(0, devices - 1)]
    pltpu.make_async_copy(others, others, inbox_sem).wait()

    mine = jnp.zeros((owned, 128), F32)
    every = jnp.zeros((owned, 128), F32)
    for q in range(groups):
        mine = mine + inbox_ref[q * across + me_s]
        for s in range(across):
            every = every + inbox_ref[q * across + s]
    mean = jnp.sum(jnp.where(small == 2 * count, every, 0.0), axis=1, keepdims=True)
    mean = mean / (shocks * across)
    part = jnp.concatenate([pd_all[me_p]] * shocks + own + [rest], axis=1) * mine
    for s in range(shocks):
        adjustment = jnp.sum(jnp.where(of_shock(s), part, 0.0), axis=1, keepdims=True)
        mine = jnp.where(small == 2 * count + 1 + shocks + s, adjustment - mean, mine)
    out_ref[...] = mine
    pltpu.make_async_copy(others, others, post_sem).wait()


def split(mine_ref, profile_ref, xva_ref, total_ref):
    owned, shocks, dates = profile_ref.shape[1:]
    count = dates * shocks
    mine = mine_ref[...]
    for half in range(2):
        for s in range(shocks):
            at = half * count + s * dates
            profile_ref[half, :, s, :] = mine[:, at : at + dates]
    row = lax.broadcasted_iota(jnp.int32, (owned, owned), 0)
    diagonal = row == lax.broadcasted_iota(jnp.int32, (owned, owned), 1)
    at = 2 * count + 1
    total_ref[...] = mine[0:1, at : at + shocks]
    for s in range(shocks):
        column = mine[:, at + shocks + s : at + shocks + s + 1]
        xva_ref[s : s + 1, :] = jnp.sum(
            jnp.where(diagonal, column, 0.0), axis=0, keepdims=True
        )


def on_device(
    factors,
    trade_weights,
    payoff_terms,
    set_blocks,
    shock_pick,
    shock_scale,
    shock_shift,
    discount,
    set_pd,
    own_pd,
):
    sets = set_blocks.shape[0]
    owned = set_pd.shape[0]
    count, dates, paths = factors.shape
    shocks = shock_pick.shape[0]
    groups = lax.axis_size("pa")
    across = lax.axis_size("sa")
    local = trade_weights.shape[1]
    vmem = pl.BlockSpec(memory_space=pltpu.VMEM)
    hbm = pl.BlockSpec(memory_space=pltpu.HBM)
    result = pl.pallas_call(
        functools.partial(kernel, groups, across),
        out_shape=jax.ShapeDtypeStruct((owned, 128), F32),
        in_specs=[hbm] * 10,
        out_specs=vmem,
        scratch_shapes=[
            pltpu.SMEM(shock_pick.shape, jnp.int32),
            pltpu.VMEM(factors.shape, BF),
            pltpu.VMEM((1, sets), jnp.int32),
            pltpu.VMEM(shock_scale.shape, F32),
            pltpu.VMEM(shock_shift.shape, F32),
            pltpu.VMEM(discount.shape, BF),
            pltpu.VMEM((1, dates), F32),
            pltpu.VMEM((count * dates, paths), F32),
            pltpu.VMEM((KDIM, dates * shocks * paths), BF),
            pltpu.VMEM((local, KDIM), BF),
            pltpu.VMEM((sets, local), BF),
            pltpu.VMEM((sets, dates * shocks * paths), F32),
            pltpu.VMEM((groups,) + trade_weights.shape, BF),
            pltpu.VMEM((groups,) + payoff_terms.shape, BF),
            pltpu.VMEM((groups,) + set_pd.shape, F32),
            pltpu.VMEM((groups, owned, 128), F32),
            pltpu.VMEM((groups * across, owned, 128), F32),
            pltpu.SemaphoreType.DMA((3, groups)),
            pltpu.SemaphoreType.DMA((3, groups)),
            pltpu.SemaphoreType.DMA,
            pltpu.SemaphoreType.DMA,
            pltpu.SemaphoreType.DMA((7,)),
        ],
        compiler_params=pltpu.CompilerParams(
            collective_id=0, has_side_effects=True
        ),
    )(
        shock_pick,
        factors,
        trade_weights,
        payoff_terms,
        set_blocks[None, :],
        shock_scale,
        shock_shift,
        discount,
        set_pd,
        own_pd[None, :],
    )
    profile, set_xva, total_xva = pl.pallas_call(
        split,
        out_shape=(
            jax.ShapeDtypeStruct((2, owned, shocks, dates), F32),
            jax.ShapeDtypeStruct((shocks, owned), F32),
            jax.ShapeDtypeStruct((1, shocks), F32),
        ),
        in_specs=[vmem],
        out_specs=(vmem, vmem, vmem),
    )(result)
    return (profile.transpose(0, 1, 3, 2), set_xva.T, total_xva[0])


def solution(mesh):
    return jax.shard_map(
        on_device,
        mesh=mesh,
        in_specs=(
            P(None, None, "pa"),
            P(None, "pa"),
            P(None, "pa"),
            P(),
            P("sa"),
            P(),
            P(),
            P(None, "pa"),
            P("pa", None),
            P(),
        ),
        out_specs=(P(None, "pa", None, "sa"), P("pa", "sa"), P("sa")),
        check_vma=False,
    )
```

```python
import functools
import math

import jax
import jax.numpy as jnp
from jax import lax
from jax.experimental import pallas as pl
from jax.experimental.pallas import tpu as pltpu
from jax.sharding import PartitionSpec as P

UNIT_SCALE = 0.0625
LOG2E = 1.0 / math.log(2.0)
BLOCK = 128
BF = jnp.bfloat16
F32 = jnp.float32
CEIL = 100.0
KDIM = 128
SUB = 128


def pick_column(library_ref, row):
    count, width = library_ref.shape
    rows = lax.broadcasted_iota(jnp.int32, (count, width), 0)
    line = jnp.sum(jnp.where(rows == row, library_ref[...], 0.0), axis=0, keepdims=True)
    square = jnp.broadcast_to(line, (width, width))
    eye = lax.broadcasted_iota(jnp.int32, (width, width), 0) == lax.broadcasted_iota(
        jnp.int32, (width, width), 1
    )
    return jnp.sum(jnp.where(eye, square, 0.0), axis=1, keepdims=True)


def shock_rows(factor_ref, pick_ref, scale_ref, shift_ref, wide_ref, shocked_ref):
    factors, dates, paths = factor_ref.shape
    shocks = pick_ref.shape[0]
    for k in range(factors):
        wide_ref[k * dates : (k + 1) * dates, :] = factor_ref[k].astype(F32)
    rest = shocked_ref.shape[0] - factors
    ones = lax.broadcasted_iota(jnp.int32, (rest, shocked_ref.shape[1]), 0) < 2
    shocked_ref[factors:, :] = jnp.where(ones, 1.0, 0.0).astype(BF)
    for s in range(shocks):
        scale = pick_column(scale_ref, pick_ref[s]) * LOG2E
        shift = pick_column(shift_ref, pick_ref[s]) * LOG2E
        scale = jnp.broadcast_to(scale, (factors, paths))
        shift = jnp.broadcast_to(shift, (factors, paths))
        for d in range(dates):
            line = wide_ref[pl.ds(d, factors, stride=dates), :]
            at = (d * shocks + s) * paths
            shocked_ref[:factors, at : at + paths] = (scale * line + shift).astype(BF)


def load_trades(weights, terms, factors):
    strike = terms[1:2].astype(F32) * LOG2E
    high = strike.astype(BF).astype(F32)
    low = strike - high
    width = weights.shape[1]
    row = lax.broadcasted_iota(jnp.int32, (KDIM - factors, width), 0)
    tail = jnp.where(row == 0, high, jnp.where(row == 1, low, 0.0)).astype(BF)
    return jnp.concatenate([weights, tail], axis=0).T


def partner(me, step, groups):
    if groups & (groups - 1):
        return lax.rem(me + step, groups)
    other, bit = 0, 1
    while bit < groups:
        other = other + lax.rem(me // bit + step // bit, 2) * bit
        bit = bit * 2
    return other


def send(source, target, send_sem, recv_sem, place):
    return pltpu.make_async_remote_copy(
        src_ref=source,
        dst_ref=target,
        send_sem=send_sem,
        recv_sem=recv_sem,
        device_id=place,
        device_id_type=pl.DeviceIdType.MESH,
    )


def kernel(
    groups,
    lanes_across,
    pick_hbm,
    factor_hbm,
    weight_hbm,
    term_hbm,
    block_hbm,
    scale_hbm,
    shift_hbm,
    discount_hbm,
    pd_hbm,
    own_hbm,
    out_ref,
    pick_ref,
    factor_ref,
    block_ref,
    scale_ref,
    shift_ref,
    discount_ref,
    own_ref,
    wide_ref,
    shocked_ref,
    loading_ref,
    member_ref,
    net_ref,
    weight_all,
    term_all,
    pd_all,
    message_ref,
    inbox_ref,
    send_sem,
    recv_sem,
    post_sem,
    inbox_sem,
    load_sem,
):
    factors, dates, paths = factor_ref.shape
    shocks = pick_ref.shape[0]
    local = weight_hbm.shape[1]
    sets = block_ref.shape[1]
    owned = pd_hbm.shape[0]
    across = lanes_across
    devices = groups * across
    me_p = lax.axis_index("pa")
    me_s = lax.axis_index("sa")
    me = me_p * across + me_s
    barrier = pltpu.get_barrier_semaphore()

    def greet(place):
        pl.semaphore_signal(
            barrier, inc=1, device_id=place, device_id_type=pl.DeviceIdType.MESH
        )

    for step in range(1, groups):
        greet((lax.rem(me_p + step, groups), me_s))
    for step in range(1, across):
        greet((me_p, lax.rem(me_s + step, across)))

    parts = ((weight_hbm, weight_all), (term_hbm, term_all), (pd_hbm, pd_all))
    early = [
        pltpu.make_async_copy(source, target, load_sem.at[n])
        for n, (source, target) in enumerate(
            (
                (pick_hbm, pick_ref),
                (scale_hbm, scale_ref),
                (shift_hbm, shift_ref),
                (factor_hbm, factor_ref),
                (block_hbm, block_ref),
                (discount_hbm, discount_ref),
                (own_hbm, own_ref),
            )
        )
    ]
    for copy in early:
        copy.start()
    for n, (source, target) in enumerate(parts):
        pltpu.make_async_copy(source, target.at[me_p], recv_sem.at[n, me_p]).start()

    def gather(step):
        other = partner(me_p, step if not groups & (groups - 1) else groups - step, groups)
        return [
            send(
                target.at[me_p],
                target.at[me_p],
                send_sem.at[n],
                recv_sem.at[n, me_p],
                (other, me_s),
            )
            for n, (source, target) in enumerate(parts)
        ]

    for n, (source, target) in enumerate(parts):
        pltpu.make_async_copy(source, target.at[me_p], recv_sem.at[n, me_p]).wait()
    pl.semaphore_wait(barrier, groups + across - 2)
    for step in range(1, groups):
        for copy in gather(step):
            copy.start()
    for copy in early:
        copy.wait()
    shock_rows(factor_ref, pick_ref, scale_ref, shift_ref, wide_ref, shocked_ref)

    m = lax.broadcasted_iota(jnp.int32, (sets, sets), 0)
    j = lax.broadcasted_iota(jnp.int32, (sets, sets), 1)
    counts = jnp.broadcast_to(block_ref[...].astype(F32), (sets, sets))
    ends = jnp.sum(jnp.where(j <= m, counts, 0.0), axis=1, keepdims=True) * BLOCK
    begins = jnp.sum(jnp.where(j < m, counts, 0.0), axis=1, keepdims=True) * BLOCK
    net_ref[...] = jnp.zeros_like(net_ref)
    wide = shocks * paths
    unroll = next(n for n in (16, 8, 4, 2, 1) if dates % n == 0)
    sub = min(SUB, local)

    def one_slot(step, _):
        slot = partner(me_p, step, groups)

        @pl.when(step > 0)
        def _():
            for n, (source, target) in enumerate(parts):
                pltpu.make_async_copy(source, target.at[slot], recv_sem.at[n, slot]).wait()

        terms = term_all[slot]
        loading_ref[...] = load_trades(weight_all[slot], terms, factors)
        ids = lax.broadcasted_iota(jnp.int32, (sets, local), 1) + slot * local
        ids = ids.astype(F32)
        notional = jnp.broadcast_to(terms[0:1].astype(F32), (sets, local))
        inside = jnp.logical_and(ids >= begins, ids < ends)
        member_ref[...] = jnp.where(inside, notional, 0.0).astype(BF)

        def some_dates(turn, _):
            for d in range(unroll):
                at = pl.multiple_of((turn * unroll + d) * wide, wide)
                columns = shocked_ref[:, pl.ds(at, wide)]
                values = []
                for r in range(0, local, sub):
                    part = loading_ref[r : r + sub, :]
                    u = jnp.dot(part, columns, preferred_element_type=F32)
                    grown = jnp.exp2(jnp.minimum(u, CEIL))
                    values.append(jnp.maximum(jnp.log2(grown + 1.0), u).astype(BF))
                whole = jnp.concatenate(values, axis=0)
                net_ref[:, pl.ds(at, wide)] += jnp.dot(
                    member_ref[...], whole, preferred_element_type=F32
                )
            return 0

        lax.fori_loop(0, dates // unroll, some_dates, 0)
        return 0

    lax.fori_loop(0, groups, one_slot, 0)

    count = dates * shocks
    lane = lax.broadcasted_iota(jnp.int32, (sets, 128), 1)
    sums = jnp.zeros((sets, 128), F32)
    total_paths = paths * groups
    for d in range(dates):
        cheap = discount_ref[d : d + 1, :].astype(F32) * (UNIT_SCALE * math.log(2.0))
        for s in range(shocks):
            at = d * wide + s * paths
            exposure = net_ref[:, at : at + paths] * cheap
            up = jnp.sum(jnp.maximum(exposure, 0.0), axis=1, keepdims=True)
            down = jnp.sum(jnp.minimum(exposure, 0.0), axis=1, keepdims=True)
            sums = jnp.where(lane == s * dates + d, up, sums)
            sums = jnp.where(lane == count + s * dates + d, down, sums)
    sums = sums / total_paths

    rest = jnp.zeros((owned, 128 - 2 * count), F32)
    own = [jnp.broadcast_to(own_ref[...], (owned, dates))] * shocks
    small = lax.broadcasted_iota(jnp.int32, (owned, 128), 1)

    def of_shock(s):
        up = jnp.logical_and(small >= s * dates, small < (s + 1) * dates)
        down = jnp.logical_and(small >= count + s * dates, small < count + (s + 1) * dates)
        return jnp.logical_or(up, down)

    totals = [jnp.zeros((1, 1), F32)] * shocks
    blocks = []
    for q in range(groups):
        rows = sums[q * owned : (q + 1) * owned, :]
        prices = jnp.concatenate([pd_all[q]] * shocks + own + [rest], axis=1)
        part = prices * rows
        both = jnp.sum(part, axis=1, keepdims=True)
        blocks.append(jnp.where(small == 2 * count, both, rows))
        for s in range(shocks):
            picked = jnp.sum(jnp.where(of_shock(s), part, 0.0), axis=1, keepdims=True)
            totals[s] = totals[s] + jnp.sum(picked, axis=0, keepdims=True)
    for q in range(groups):
        block = blocks[q]
        for s in range(shocks):
            block = jnp.where(small == 2 * count + 1 + s, totals[s], block)
        message_ref[q] = block
    inbox_ref[me] = message_ref[me_p]

    for far_p in reversed(range(groups)):
        for far_s in reversed(range(across)):
            if far_p + far_s:
                other_p = partner(me_p, far_p, groups)
                send(
                    message_ref.at[other_p],
                    inbox_ref.at[me],
                    post_sem,
                    inbox_sem,
                    (other_p, partner(me_s, far_s, across)),
                ).start()
    for n, (source, target) in enumerate(parts):
        gone = target.at[pl.ds(0, groups - 1)]
        pltpu.make_async_copy(gone, gone, send_sem.at[n]).wait()
    others = inbox_ref.at[pl.ds(0, devices - 1)]
    pltpu.make_async_copy(others, others, inbox_sem).wait()

    mine = jnp.zeros((owned, 128), F32)
    every = jnp.zeros((owned, 128), F32)
    for q in range(groups):
        mine = mine + inbox_ref[q * across + me_s]
        for s in range(across):
            every = every + inbox_ref[q * across + s]
    mean = jnp.sum(jnp.where(small == 2 * count, every, 0.0), axis=1, keepdims=True)
    mean = mean / (shocks * across)
    part = jnp.concatenate([pd_all[me_p]] * shocks + own + [rest], axis=1) * mine
    for s in range(shocks):
        adjustment = jnp.sum(jnp.where(of_shock(s), part, 0.0), axis=1, keepdims=True)
        mine = jnp.where(small == 2 * count + 1 + shocks + s, adjustment - mean, mine)
    out_ref[...] = mine
    pltpu.make_async_copy(others, others, post_sem).wait()


def split(mine_ref, profile_ref, xva_ref, total_ref):
    owned, shocks, dates = profile_ref.shape[1:]
    count = dates * shocks
    mine = mine_ref[...]
    for half in range(2):
        for s in range(shocks):
            at = half * count + s * dates
            profile_ref[half, :, s, :] = mine[:, at : at + dates]
    row = lax.broadcasted_iota(jnp.int32, (owned, owned), 0)
    diagonal = row == lax.broadcasted_iota(jnp.int32, (owned, owned), 1)
    at = 2 * count + 1
    total_ref[...] = mine[0:1, at : at + shocks]
    for s in range(shocks):
        column = mine[:, at + shocks + s : at + shocks + s + 1]
        xva_ref[s : s + 1, :] = jnp.sum(
            jnp.where(diagonal, column, 0.0), axis=0, keepdims=True
        )


def on_device(
    factors,
    trade_weights,
    payoff_terms,
    set_blocks,
    shock_pick,
    shock_scale,
    shock_shift,
    discount,
    set_pd,
    own_pd,
):
    sets = set_blocks.shape[0]
    owned = set_pd.shape[0]
    count, dates, paths = factors.shape
    shocks = shock_pick.shape[0]
    groups = lax.axis_size("pa")
    across = lax.axis_size("sa")
    local = trade_weights.shape[1]
    vmem = pl.BlockSpec(memory_space=pltpu.VMEM)
    hbm = pl.BlockSpec(memory_space=pltpu.HBM)
    result = pl.pallas_call(
        functools.partial(kernel, groups, across),
        out_shape=jax.ShapeDtypeStruct((owned, 128), F32),
        in_specs=[hbm] * 10,
        out_specs=vmem,
        scratch_shapes=[
            pltpu.SMEM(shock_pick.shape, jnp.int32),
            pltpu.VMEM(factors.shape, BF),
            pltpu.VMEM((1, sets), jnp.int32),
            pltpu.VMEM(shock_scale.shape, F32),
            pltpu.VMEM(shock_shift.shape, F32),
            pltpu.VMEM(discount.shape, BF),
            pltpu.VMEM((1, dates), F32),
            pltpu.VMEM((count * dates, paths), F32),
            pltpu.VMEM((KDIM, dates * shocks * paths), BF),
            pltpu.VMEM((local, KDIM), BF),
            pltpu.VMEM((sets, local), BF),
            pltpu.VMEM((sets, dates * shocks * paths), F32),
            pltpu.VMEM((groups,) + trade_weights.shape, BF),
            pltpu.VMEM((groups,) + payoff_terms.shape, BF),
            pltpu.VMEM((groups,) + set_pd.shape, F32),
            pltpu.VMEM((groups, owned, 128), F32),
            pltpu.VMEM((groups * across, owned, 128), F32),
            pltpu.SemaphoreType.DMA((3,)),
            pltpu.SemaphoreType.DMA((3, groups)),
            pltpu.SemaphoreType.DMA,
            pltpu.SemaphoreType.DMA,
            pltpu.SemaphoreType.DMA((7,)),
        ],
        compiler_params=pltpu.CompilerParams(
            collective_id=0, has_side_effects=True
        ),
    )(
        shock_pick,
        factors,
        trade_weights,
        payoff_terms,
        set_blocks[None, :],
        shock_scale,
        shock_shift,
        discount,
        set_pd,
        own_pd[None, :],
    )
    profile, set_xva, total_xva = pl.pallas_call(
        split,
        out_shape=(
            jax.ShapeDtypeStruct((2, owned, shocks, dates), F32),
            jax.ShapeDtypeStruct((shocks, owned), F32),
            jax.ShapeDtypeStruct((1, shocks), F32),
        ),
        in_specs=[vmem],
        out_specs=(vmem, vmem, vmem),
    )(result)
    return (profile.transpose(0, 1, 3, 2), set_xva.T, total_xva[0])


def solution(mesh):
    return jax.shard_map(
        on_device,
        mesh=mesh,
        in_specs=(
            P(None, None, "pa"),
            P(None, "pa"),
            P(None, "pa"),
            P(),
            P("sa"),
            P(),
            P(),
            P(None, "pa"),
            P("pa", None),
            P(),
        ),
        out_specs=(P(None, "pa", None, "sa"), P("pa", "sa"), P("sa")),
        check_vma=False,
    )
```
